128 devices in a mesh: data: 1, inner: 64 (over z, y, x), stage: 2 (over core).
Axes of the slice: x: 4, y: 4, z: 4, core: 2. Of those that a mesh axis runs over, the one named last changes fastest.
Arguments:
- x: bfloat16 [16, 4096, 1024], P(('data', 'stage'), 'inner')
- g: bfloat16 [16, 4096, 1024], P(('data', 'stage'), 'inner')
- w1: bfloat16 [1, 2, 1024, 4096], P(None, 'stage')
- w2: bfloat16 [1, 2, 4096, 1024], P(None, 'stage')
Outputs:
- output 1: bfloat16 [16, 4096, 1024], P(('data', 'stage'), 'inner')
- output 2: bfloat16 [16, 4096, 1024], P(('data', 'stage'), 'inner')
- output 3: float32 [1, 2, 1024, 4096], P('data', 'stage')
- output 4: float32 [1, 2, 4096, 1024], P('data', 'stage')
All inputs are finite; a program needn't handle non-finite values.
Results may differ from the reference program's by a relative error of at most 0.00491169.
Values are sent between devices in bfloat16 or wider.
A program may use at most 1 GiB of HBM per device.

```python
import jax
import jax.numpy as jnp
from jax import lax

D = 1024
FF = 4096
V = 1
K = 1
STAGE = 2
MICRO = 16
B = 4096

LAYERS = V * STAGE * K


def setup_inputs(seed: int = 0, part: int = 0) -> dict:
    key = jax.random.PRNGKey(seed)
    kbase, kshared = jax.random.split(key)
    kx, kg = jax.random.split(jax.random.fold_in(kbase, part))
    k1, k2 = jax.random.split(kshared)
    x = jax.random.normal(kx, (MICRO, B, D), jnp.float32).astype(jnp.bfloat16)
    g = jax.random.normal(kg, (MICRO, B, D), jnp.float32).astype(jnp.bfloat16)
    w1 = (jax.random.normal(k1, (V, STAGE * K, D, FF), jnp.float32) * D ** -0.5).astype(jnp.bfloat16)
    w2 = (jax.random.normal(k2, (V, STAGE * K, FF, D), jnp.float32) * (2.0 * (FF * LAYERS) ** -0.5)).astype(jnp.bfloat16)
    return {"x": x, "g": g, "w1": w1, "w2": w2}


def _gelu(t):
    return jax.nn.gelu(t, approximate=True)


def _layer_fwd(h, w1, w2):
    z = jnp.dot(h, w1, preferred_element_type=jnp.float32)
    a = _gelu(z).astype(jnp.bfloat16)
    u = jnp.dot(a, w2, preferred_element_type=jnp.float32)
    return (h.astype(jnp.float32) + u).astype(jnp.bfloat16)


def _layer_bwd(h, dh, w1, w2):
    z = jnp.dot(h, w1, preferred_element_type=jnp.float32)
    a32, gelu_vjp = jax.vjp(_gelu, z)
    a = a32.astype(jnp.bfloat16)
    dw2 = jnp.dot(a.T, dh, preferred_element_type=jnp.float32)
    da = jnp.dot(dh, w2.T, preferred_element_type=jnp.float32)
    dz = gelu_vjp(da)[0].astype(jnp.bfloat16)
    dw1 = jnp.dot(h.T, dz, preferred_element_type=jnp.float32)
    dh_prev = (dh.astype(jnp.float32) + jnp.dot(dz, w1.T, preferred_element_type=jnp.float32)).astype(jnp.bfloat16)
    return dh_prev, dw1, dw2


def reference(x, g, w1, w2):
    w1s = w1.reshape(LAYERS, D, FF)
    w2s = w2.reshape(LAYERS, FF, D)

    def one_micro(acc, xg):
        dw1_acc, dw2_acc = acc
        xm, gm = xg

        def fwd(h, w):
            return _layer_fwd(h, w[0], w[1]), h

        y, hs = lax.scan(fwd, xm, (w1s, w2s))

        def bwd(dh, inp):
            h, a, b = inp
            dh_prev, d1, d2 = _layer_bwd(h, dh, a, b)
            return dh_prev, (d1, d2)

        dx, (d1s, d2s) = lax.scan(bwd, gm, (hs, w1s, w2s), reverse=True)
        return (dw1_acc + d1s, dw2_acc + d2s), (y, dx)

    init = (jnp.zeros((LAYERS, D, FF), jnp.float32), jnp.zeros((LAYERS, FF, D), jnp.float32))
    (dw1, dw2), (y, dx) = lax.scan(one_micro, init, (x, g))
    return y, dx, dw1.reshape(w1.shape), dw2.reshape(w2.shape)
```

```python
import functools

import jax
import jax.numpy as jnp
from jax import lax
from jax.experimental import pallas as pl
from jax.experimental.pallas import tpu as pltpu
from jax.sharding import PartitionSpec as P

MESH = pl.DeviceIdType.MESH
F32 = jnp.float32
BF16 = jnp.bfloat16
N = 4
STEPS = 14
OWN = 6
FAR = 4

_K = 0.7978845608028654
_C = 0.044715


def _gelu_and_slope(z):
    z2 = z * z
    t = jnp.tanh(z * (_K + (_K * _C) * z2))
    cdf = 0.5 + 0.5 * t
    slope = cdf + (z * (1.0 - t * t)) * (0.5 * _K + (1.5 * _K * _C) * z2)
    return z * cdf, slope


def _dot(a, b, dims=((1,), (0,))):
    return lax.dot_general(a, b, (dims, ((), ())), preferred_element_type=F32)


def _ds(start, size):
    return pl.ds(pl.multiple_of(start, size), size)


def _kernel(
    RB, F,
    x_ref, g_ref, w1_ref, w2_ref,
    y_ref, dx_ref, o1_ref, o2_ref, spill_ref,
    w1, w2, LT, R, hv, BUF, ST, Z, YS,
    SA1, HA1, SB1, HB1, RR1,
    SA2, HA2, SB2, HB2, RR2,
    SA3, HA3, SB3, HB3,
    AG,
    ld_sem, xg_send, xg_recv, ex_send, ex_recv, sp_w, sp_r, out_send, out_recv, out_loc,
    msend, mrecv, own_sem, near_sem, opp_sem,
):
    D = 4 * RB
    CW = RB
    HW = CW // 2
    TU = 2 * RB
    FT = F // 8
    n2 = (F // D) * (D // CW)
    n_parts = n2 + F // CW
    NQ = (n_parts + 2) // 3
    NT = NQ + STEPS - 1
    rows = (RB, RB // 4, RB // 16)

    st = lax.axis_index("stage")
    me = lax.axis_index("inner")
    c = (me % N, (me // N) % N, me // (N * N))
    stride = (1, N, N * N)

    def at(dim, delta):
        return (c[dim] + delta) % N

    nbr = [
        tuple(me + (at(dim, delta) - c[dim]) * stride[dim] for delta in (1, -1))
        for dim in range(3)
    ]

    def remote(src, dst, ss, rs, to, core):
        return pltpu.make_async_remote_copy(
            src_ref=src, dst_ref=dst, send_sem=ss, recv_sem=rs, device_id=(0, to, core), device_id_type=MESH
        )

    def await_(ref, sem):
        pltpu.make_async_copy(ref, ref, sem).wait()

    partner = 1 - st

    own_rows = _ds(st * TU, TU)
    lw1 = pltpu.make_async_copy(w1_ref, w1, ld_sem.at[0])
    lw2 = pltpu.make_async_copy(w2_ref, w2, ld_sem.at[1])

    barrier = pltpu.get_barrier_semaphore()
    pl.semaphore_signal(barrier, inc=1, device_id=(0, me, partner), device_id_type=MESH)
    for dim in range(3):
        for to in nbr[dim]:
            pl.semaphore_signal(barrier, inc=1, device_id=(0, to, st), device_id_type=MESH)

    @pl.when(st == 0)
    def _():
        pltpu.make_async_copy(x_ref, hv.at[own_rows, :], ld_sem.at[2]).start()
        lw1.start()
        lw2.start()

    @pl.when(st == 1)
    def _():
        pltpu.make_async_copy(g_ref, R.at[own_rows, pl.ds(0, D)], ld_sem.at[2]).start()
        lw2.start()
        lw1.start()

    pl.semaphore_wait(barrier, 7)

    def x_over():
        return remote(x_ref, hv.at[own_rows, :], xg_send, xg_recv, me, partner)

    def g_over():
        return remote(g_ref, R.at[own_rows, pl.ds(0, D)], xg_send, xg_recv, me, partner)

    def spill_w(k):
        return pltpu.make_async_copy(ST.at[k % 2], spill_ref.at[k], sp_w.at[k % 2])

    def spill_r(k):
        return pltpu.make_async_copy(spill_ref.at[k], ST.at[k % 2], sp_r.at[k % 2])

    def urows(u):
        return _ds(u * TU, TU)

    def h_transposed(u):
        @pl.loop(0, 4)
        def _(k):
            LT[_ds(F + k * RB, RB), urows(u)] = hv[urows(u), _ds(k * RB, RB)].T

    def put_a(u, j, a):
        LT[_ds(j * FT, FT), urows(u)] = a.T

    def put_dz(u, j, dz):
        R[urows(u), _ds(D + j * FT, FT)] = dz

    def z_tile(u, j):
        return _dot(hv[urows(u), :], w1[:, _ds(j * FT, FT)])

    def da_tile(u, j):
        return _dot(R[urows(u), pl.ds(0, D)], w2[_ds(j * FT, FT), :], ((1,), (1,)))

    def dh_tile(u, ct):
        acc = _dot(R[urows(u), pl.ds(D, F)], w1[_ds(ct * RB, RB), :], ((1,), (1,)))
        return (R[urows(u), _ds(ct * RB, RB)].astype(F32) + acc).astype(BF16)

    def across(u, ct, val, dst):
        for r in range(2):
            SB1[ct * 2 + r] = val[r * RB : (r + 1) * RB]
        for r in range(2):
            remote(
                SB1.at[ct * 2 + r], dst.at[_ds(u * TU + r * RB, RB), _ds(ct * RB, RB)],
                ex_send.at[u], ex_recv.at[u], me, partner,
            ).start()

    def across_sent(u):
        await_(SB1.at[pl.ds(0, 8)], ex_send.at[u])

    @pl.when(st == 0)
    def _():
        g_over().start()
        pltpu.make_async_copy(x_ref, hv.at[own_rows, :], ld_sem.at[2]).wait()
        lw1.wait()

        @pl.loop(0, 2)
        def _(u):
            @pl.when(u == 1)
            def _():
                await_(hv.at[pl.ds(0, TU), :], xg_recv)

            Z[0] = z_tile(u, 0)
            h_transposed(u)

            def finish(j, z):
                a, slope = _gelu_and_slope(z)
                a = a.astype(BF16)
                for r in range(2):
                    for k in range(FT // CW):
                        BUF[r * (F // CW) + j * (FT // CW) + k] = a[r * RB : (r + 1) * RB, k * CW : (k + 1) * CW]
                put_a(u, j, a)
                return slope

            def spill(j, slope):
                k = u * 8 + j
                ST[k % 2] = slope
                spill_w(k).start()

            @pl.loop(0, 7)
            def _(j):
                @pl.when(u * 8 + j >= 2)
                def _():
                    spill_w(u * 8 + j).wait()

                Z[(j + 1) % 2] = z_tile(u, j + 1)
                spill(j, finish(j, Z[j % 2]))

            spill_w(u * 8 + 7).wait()
            spill(7, finish(7, Z[1]))

            @pl.when(u == 0)
            def _():
                lw2.wait()

            @pl.when(u == 1)
            def _():
                across_sent(0)

            @pl.loop(0, 4)
            def _(ct):
                a = jnp.concatenate(
                    [jnp.concatenate([BUF[r * (F // CW) + k] for k in range(F // CW)], axis=1) for r in range(2)], axis=0
                )
                acc = _dot(a, w2[:, _ds(ct * RB, RB)])
                h1 = (hv[urows(u), _ds(ct * RB, RB)].astype(F32) + acc).astype(BF16)
                across(u, ct, h1, hv)

        spill_w(0).wait()
        spill_w(1).wait()
        across_sent(1)
        g_over().wait_send()
        spill_r(0).start()

        @pl.loop(0, 2)
        def _(u):
            await_(SB1.at[pl.ds(0, 8)], ex_recv.at[u])
            Z[0] = da_tile(u, 0)

            def finish(k, j, da):
                spill_r(k).wait()
                put_dz(u, j, (da * ST[k % 2]).astype(BF16))

            @pl.loop(0, 7)
            def _(j):
                k = u * 8 + j
                spill_r(k + 1).start()
                Z[(j + 1) % 2] = da_tile(u, j + 1)
                finish(k, j, Z[j % 2])

            @pl.when(u == 0)
            def _():
                spill_r(8).start()

            finish(u * 8 + 7, 7, Z[1])

    @pl.when(st == 1)
    def _():
        x_over().start()
        pltpu.make_async_copy(g_ref, R.at[own_rows, pl.ds(0, D)], ld_sem.at[2]).wait()
        lw2.wait()

        @pl.loop(0, 2)
        def _(i):
            @pl.when(i == 1)
            def _():
                await_(hv.at[pl.ds(0, TU), :], xg_recv)

            @pl.loop(0, 8)
            def _(j):
                k = (1 - i) * 8 + j

                @pl.when(i * 8 + j >= 2)
                def _():
                    spill_w(k).wait()

                ST[k % 2] = da_tile(1 - i, j)
                spill_w(k).start()

        spill_w(0).wait()
        spill_w(1).wait()
        lw1.wait()
        x_over().wait_send()
        spill_r(0).start()

        @pl.loop(0, 2)
        def _(u):
            await_(SB1.at[pl.ds(0, 8)], ex_recv.at[u])
            Z[0] = z_tile(u, 0)
            h_transposed(u)

            def finish(k, j, z):
                spill_r(k).wait()
                a, slope = _gelu_and_slope(z)
                put_a(u, j, a.astype(BF16))
                put_dz(u, j, (ST[k % 2] * slope).astype(BF16))

            @pl.loop(0, 7)
            def _(j):
                k = u * 8 + j
                spill_r(k + 1).start()
                Z[(j + 1) % 2] = z_tile(u, j + 1)
                finish(k, j, Z[j % 2])

            @pl.when(u == 0)
            def _():
                spill_r(8).start()

            finish(u * 8 + 7, 7, Z[1])

            @pl.when(u == 1)
            def _():
                across_sent(0)

            @pl.loop(0, 4)
            def _(ct):
                across(u, ct, dh_tile(u, ct), R)

        across_sent(1)

    def out_tile(k):
        u, ct, s = k // 4, k % 4, k % 2

        def to(ref, local):
            dst = ref.at[:, _ds(ct * RB, RB)]
            if local:
                return pltpu.make_async_copy(YS.at[s], dst, out_loc.at[s])
            return remote(YS.at[s], dst, out_send.at[s], out_recv, me, partner)

        def sent(k):
            @pl.when(k // 4 == st)
            def _():
                await_(YS.at[s], out_loc.at[s])

            @pl.when(k // 4 != st)
            def _():
                await_(YS.at[s], out_send.at[s])

        @pl.when(k >= 2)
        def _():
            sent(k - 2)

        @pl.when(k < 8)
        def _():
            @pl.when(st == 0)
            def _():
                YS[s] = dh_tile(u, ct)

                @pl.when(u == 0)
                def _():
                    to(dx_ref, True).start()

                @pl.when(u == 1)
                def _():
                    to(dx_ref, False).start()

            @pl.when(st == 1)
            def _():
                acc = _dot(LT[pl.ds(0, F), urows(u)], w2[:, _ds(ct * RB, RB)], ((0,), (0,)))
                YS[s] = (hv[urows(u), _ds(ct * RB, RB)].astype(F32) + acc).astype(BF16)

                @pl.when(u == 0)
                def _():
                    to(y_ref, False).start()

                @pl.when(u == 1)
                def _():
                    to(y_ref, True).start()

    def axis(j, level):
        return (j + level) % 3

    def part(q, j):
        return jnp.minimum(3 * q + j, n_parts - 1)

    def lrow(n, r):
        return jnp.where(n < n2, (n // 4) * D + r * RB, F + r * RB)

    def rcol(n):
        return jnp.where(n < n2, (n % 4) * CW, D + (n - n2) * CW)

    def product(q, j, r):
        n = part(q, j)
        return _dot(LT[_ds(lrow(n, r), RB), :], R[:, _ds(rcol(n), CW)])

    def send(kind, q, j, level, way, src, dst):
        s = q % 2
        remote(src, dst, msend.at[kind, s], mrecv.at[kind, s], nbr[axis(j, level)][way], st).start()

    def came(kind, q, ref):
        await_(ref, mrecv.at[kind, q % 2])

    def gone(kind, q, ref):
        await_(ref, msend.at[kind, q % 2])

    SA, HA, SB, HB = (SA1, SA2, SA3), (HA1, HA2, HA3), (SB1, SB2, SB3), (HB1, HB2, HB3)
    RR = (None, RR1, RR2)

    def sb(level, q, j, way):
        return SB[level].at[((q % 2) * 3 + j) * 2 + way]

    def block(level, q, j, delta):
        r = at(axis(j, level), delta)
        if level == 0:
            return product(q, j, r)
        return RR[level][q % 2, j, _ds(r * rows[level], rows[level]), :]

    def first(level, q):
        for j in range(3):
            SA[level][q % 2, j] = block(level, q, j, 2).astype(BF16)
        for j in range(3):
            for way in range(2):
                send(
                    2 * level, q, j, level, way,
                    SA[level].at[q % 2, j, :, pl.ds(way * HW, HW)], HA[level].at[q % 2, j, way],
                )

    def second(level, q):
        s = q % 2
        came(2 * level, q, HA[level].at[s])
        for j in range(3):
            for way in range(2):
                own = block(level, q, j, 1 - 2 * way)
                here = own[:, way * HW : (way + 1) * HW] + HA[level][s, j, way].astype(F32)
                there = own[:, (1 - way) * HW : (2 - way) * HW]
                halves = (here, there) if way == 0 else (there, here)
                SB[level][(s * 3 + j) * 2 + way] = jnp.concatenate(halves, axis=1).astype(BF16)
        for j in range(3):
            for way in range(2):
                send(2 * level + 1, q, j, level, way, sb(level, q, j, way), HB[level].at[s, j, way])
        gone(2 * level, q, SA[level].at[s])

    def third(level, q):
        s = q % 2
        came(2 * level + 1, q, HB[level].at[s])
        total = [
            block(level, q, j, 0) + (HB[level][s, j, 0].astype(F32) + HB[level][s, j, 1].astype(F32)) for j in range(3)
        ]
        gone(2 * level + 1, q, HB[level].at[s])
        return total

    def own(q, j, level, delta, half=None):
        a = at(axis(j, 1), delta if level == 1 else 0) * rows[1]
        if level == 2:
            a = a + at(axis(j, 2), delta) * rows[2]
        cols = slice(None) if half is None else pl.ds(half * HW, HW)
        return AG.at[q % OWN, j, _ds(a, rows[level]), cols]

    def span(k):
        return AG.at[0, :, pl.ds(0, k), :]

    def near(q, j, pos, half=None):
        k = ((q % FAR) * 3 + j) * 3 + pos
        return BUF.at[k] if half is None else BUF.at[k, :, pl.ds(half * HW, HW)]

    def out_copy(q, j, src, delta, sem):
        n = part(q, j)
        r = at(axis(j, 0), delta)

        @pl.when(3 * q + j < n2)
        def _():
            pltpu.make_async_copy(src, o2_ref.at[_ds((n // 4) * D + r * RB, RB), _ds((n % 4) * CW, CW)], sem).start()

        @pl.when((3 * q + j >= n2) & (3 * q + j < n_parts))
        def _():
            pltpu.make_async_copy(src, o1_ref.at[_ds(r * RB, RB), _ds((n - n2) * CW, CW)], sem).start()

    def out_done(q, j, blocks, sem):
        @pl.when(3 * q + j < n_parts)
        def _():
            await_(BUF.at[pl.ds(0, blocks)], sem)

    def s1(q):
        first(0, q)

    def s2(q):
        second(0, q)

    def s3(q):
        for j, total in enumerate(third(0, q)):
            RR1[q % 2, j] = total
        first(1, q)

    def s4(q):
        second(1, q)

    def s5(q):
        for j, total in enumerate(third(1, q)):
            RR2[q % 2, j] = total
        first(2, q)

    def s6(q):
        second(2, q)

    def s7(q):
        for j, total in enumerate(third(2, q)):
            a = at(axis(j, 1), 0) * rows[1] + at(axis(j, 2), 0) * rows[2]
            AG[q % OWN, j, _ds(a, rows[2]), :] = total.astype(BF16)
        for j in range(3):
            for way in range(2):
                send(6, q, j, 2, way, own(q, j, 2, 0), own(q, j, 2, 0))

    def s8(q):
        came(6, q, span(2 * rows[2]))
        gone(6, q, span(2 * rows[2]))
        for j in range(3):
            for way in range(2):
                blk = own(q, j, 2, 2 * way - 1, way)
                send(7, q, j, 2, way, blk, blk)

    def s9(q):
        came(7, q, span(rows[2]))
        gone(7, q, span(rows[2]))
        for j in range(3):
            for way in range(2):
                send(8, q, j, 1, way, own(q, j, 1, 0), own(q, j, 1, 0))

    def s10(q):
        came(8, q, span(2 * rows[1]))
        gone(8, q, span(2 * rows[1]))
        for j in range(3):
            for way in range(2):
                blk = own(q, j, 1, 2 * way - 1, way)
                send(9, q, j, 1, way, blk, blk)

    def s11(q):
        came(9, q, span(rows[1]))
        gone(9, q, span(rows[1]))
        for j in range(3):
            for way in range(2):
                send(10, q, j, 0, way, AG.at[q % OWN, j], near(q, j, way))
        for j in range(3):
            out_copy(q, j, AG.at[q % OWN, j], 0, own_sem.at[q % 2])

    def s12(q):
        came(10, q, BUF.at[pl.ds(0, 6)])
        gone(10, q, BUF.at[pl.ds(0, 6)])
        for j in range(3):
            for way in range(2):
                send(11, q, j, 0, way, near(q, j, way, way), near(q, j, 2, way))
        for j in range(3):
            out_done(q, j, 1, own_sem.at[q % 2])
            for way in range(2):
                out_copy(q, j, near(q, j, way), 2 * way - 1, near_sem.at[q % 2])

    def s13(q):
        came(11, q, BUF.at[pl.ds(0, 3)])
        gone(11, q, BUF.at[pl.ds(0, 3)])
        for j in range(3):
            out_done(q, j, 2, near_sem.at[q % 2])
            out_copy(q, j, near(q, j, 2), 2, opp_sem.at[q % 2])

    def s14(q):
        for j in range(3):
            out_done(q, j, 1, opp_sem.at[q % 2])

    steps = (s1, s2, s3, s4, s5, s6, s7, s8, s9, s10, s11, s12, s13, s14)

    @pl.loop(0, NT)
    def _(t):
        for k in reversed(range(STEPS)):
            q = t - k

            @pl.when((q >= 0) & (q < NQ))
            def _():
                steps[k](q)

        k = t - 6

        @pl.when((k >= 0) & (k < 10))
        def _():
            out_tile(k)

    await_(BUF.at[pl.ds(0, 8)], out_recv)


def _one(x, g, w1, w2):
    T2, D = x.shape
    F = w1.shape[1]
    RB = D // 4
    V, S = pltpu.VMEM, pltpu.SemaphoreType
    rows = (RB, RB // 4, RB // 16)

    def ring(level):
        r = rows[level]
        return [
            V((2, 3, r, RB), BF16),
            V((2, 3, 2, r, RB // 2), BF16),
            V((12, r, RB), BF16),
            V((2, 3, 2, r, RB), BF16),
        ]

    scratch = [
        V((D, F), BF16),
        V((F, D), BF16),
        V((F + D, 2 * T2), BF16),
        V((2 * T2, D + F), BF16),
        V((2 * T2, D), BF16),
        V((9 * FAR, RB, RB), BF16),
        V((2, T2, F // 8), F32),
        V((2, T2, F // 8), F32),
        V((2, T2, RB), BF16),
        *ring(0),
        V((2, 3, RB, RB), F32),
        *ring(1),
        V((2, 3, RB // 4, RB), F32),
        *ring(2),
        V((OWN, 3, RB, RB), BF16),
        S.DMA((3,)),
        S.DMA,
        S.DMA,
        S.DMA((2,)),
        S.DMA((2,)),
        S.DMA((2,)),
        S.DMA((2,)),
        S.DMA((2,)),
        S.DMA,
        S.DMA((2,)),
        S.DMA((12, 2)),
        S.DMA((12, 2)),
        S.DMA((2,)),
        S.DMA((2,)),
        S.DMA((2,)),
    ]
    hbm = pl.BlockSpec(memory_space=pl.ANY)
    sds = jax.ShapeDtypeStruct
    return pl.pallas_call(
        functools.partial(_kernel, RB, F),
        name="mlp_stack",
        out_shape=[
            sds((T2, D), BF16),
            sds((T2, D), BF16),
            sds((D, F), BF16),
            sds((F, D), BF16),
            sds((16, T2, F // 8), F32),
        ],
        in_specs=[hbm] * 4,
        out_specs=[hbm] * 5,
        scratch_shapes=scratch,
        compiler_params=pltpu.CompilerParams(
            collective_id=0, has_side_effects=True, vmem_limit_bytes=67_043_328
        ),
    )(x, g, w1, w2)


def solution(mesh):
    def body(x, g, w1, w2):
        mb, bl, d = x.shape
        f = w1.shape[-1]
        y, dx, dw1, dw2, _ = _one(x.reshape(mb * bl, d), g.reshape(mb * bl, d), w1.reshape(d, f), w2.reshape(f, d))
        return (
            y.reshape(x.shape),
            dx.reshape(x.shape),
            dw1.astype(F32).reshape(1, 1, d, f),
            dw2.astype(F32).reshape(1, 1, f, d),
        )

    tok = P(("data", "stage"), "inner", None)
    wsp = P(None, "stage", None, None)
    dsp = P("data", "stage", None, None)
    return jax.shard_map(body, mesh=mesh, in_specs=(tok, tok, wsp, wsp), out_specs=(tok, tok, dsp, dsp), check_vma=False)
```
